32 devices in a mesh: cells: 8 (over z, y), bins: 4 (over x, core).
Axes of the slice: x: 2, y: 2, z: 4, core: 2. Of those that a mesh axis runs over, the one named last changes fastest.
Arguments:
- snapshots: bfloat16 [4, 65536, 512], P('bins', 'cells'), may hold values from -150 to 150
- training: int32 [65536], P('cells'), may hold values 0 or 1
- doppler: int32 [4, 128], P('bins'), may hold values from 0 to 1023
Outputs:
- filtered: bfloat16 [4, 256, 65536], P('bins', None, 'cells')
The draws below stay inside these ranges and needn't reach their ends.
All inputs are finite; a program needn't handle non-finite values. No bound on the sum of `training` on one device may be relied on, other than what follows from the above.
Results may differ from the reference program's by a relative error of at most 0.003.
The reference program's roundings to bfloat16 on the way (of `taps`) count: a program that leaves them out, or rounds other values in their place, can miss the bound.
Values sent between devices are 32-bit elements; how exact they have to be, the bound alone decides.
A program may use at most 64 MiB of HBM per device.

```python
import jax
import jax.numpy as jnp
from jax import lax

CHANNELS = 16
PULSES = 16
DIM = 256
BINS_G = 128
NDOPP = 1024
CELLS = 65536
GROUPS = 4


def draw_snapshots(key, part):
    keys = jax.random.split(jax.random.fold_in(key, 7101), 13)
    patches = CHANNELS + PULSES
    jammers = 2
    width = 2 * DIM
    noise_part = jnp.clip(jax.random.normal(keys[0], (GROUPS, CELLS, width), jnp.float32), -4.0, 4.0)
    clutter_re = jnp.clip(jax.random.normal(keys[1], (GROUPS, CELLS, patches), jnp.float32), -4.0, 4.0) * 0.7071
    clutter_im = jnp.clip(jax.random.normal(keys[2], (GROUPS, CELLS, patches), jnp.float32), -4.0, 4.0) * 0.7071
    jam_re = jnp.clip(jax.random.normal(keys[3], (GROUPS, CELLS, jammers, PULSES), jnp.float32), -4.0, 4.0) * 0.7071
    jam_im = jnp.clip(jax.random.normal(keys[4], (GROUPS, CELLS, jammers, PULSES), jnp.float32), -4.0, 4.0) * 0.7071
    gains = jnp.exp(jax.random.uniform(keys[5], (GROUPS, 1, DIM), jnp.float32, jnp.log(0.5), jnp.log(2.0)))
    index = jnp.arange(DIM)
    chan = (index // PULSES).astype(jnp.float32)
    pulse = (index % PULSES).astype(jnp.float32)
    offset = jax.random.uniform(keys[6], (GROUPS, 1), jnp.float32, 0.0, 1.0)
    spatial = (jnp.arange(patches).astype(jnp.float32)[None, :] + offset) / patches - 0.5
    slope = jax.random.uniform(keys[7], (GROUPS, 1), jnp.float32, 0.8, 1.2)
    temporal = slope * spatial
    phase = 2.0 * jnp.pi * (spatial[:, :, None] * chan[None, None, :] + temporal[:, :, None] * pulse[None, None, :])
    patch_power = jnp.exp(jax.random.uniform(keys[8], (GROUPS, 1, patches), jnp.float32, jnp.log(0.5), jnp.log(8.0)))
    amp_re = clutter_re * jnp.sqrt(patch_power)
    amp_im = clutter_im * jnp.sqrt(patch_power)
    cosines = jnp.cos(phase)
    sines = jnp.sin(phase)
    real_sum = jnp.einsum('gnk,gkd->gnd', amp_re, cosines) - jnp.einsum('gnk,gkd->gnd', amp_im, sines)
    imag_sum = jnp.einsum('gnk,gkd->gnd', amp_re, sines) + jnp.einsum('gnk,gkd->gnd', amp_im, cosines)
    jam_angle = jax.random.uniform(keys[9], (GROUPS, jammers), jnp.float32, -0.5, 0.5)
    jam_power = jnp.exp(jax.random.uniform(keys[10], (GROUPS, 1, jammers, 1), jnp.float32, jnp.log(10.0), jnp.log(60.0)))
    chans = jnp.arange(CHANNELS).astype(jnp.float32)
    jam_phase = 2.0 * jnp.pi * jam_angle[:, :, None] * chans[None, None, :]
    jam_cos = jnp.cos(jam_phase)
    jam_sin = jnp.sin(jam_phase)
    jr = jam_re * jnp.sqrt(jam_power)
    ji = jam_im * jnp.sqrt(jam_power)
    jam_real = jnp.einsum('gnjp,gjc->gncp', jr, jam_cos) - jnp.einsum('gnjp,gjc->gncp', ji, jam_sin)
    jam_imag = jnp.einsum('gnjp,gjc->gncp', jr, jam_sin) + jnp.einsum('gnjp,gjc->gncp', ji, jam_cos)
    real_sum = real_sum + jam_real.reshape(GROUPS, CELLS, DIM)
    imag_sum = imag_sum + jam_imag.reshape(GROUPS, CELLS, DIM)
    signal = jnp.concatenate([real_sum, imag_sum], -1) + noise_part
    both_gains = jnp.concatenate([gains, gains], -1)
    rough = jnp.exp(jax.random.uniform(keys[11], (GROUPS, CELLS, 1), jnp.float32, 0.0, jnp.log(3.0)))
    place = jnp.arange(CELLS).astype(jnp.float32) / CELLS
    ranged = (0.6 + 1.4 * place)[None, :, None]
    order = jax.random.permutation(keys[12], GROUPS).astype(jnp.float32)
    level = (1.0 + 2.0 * order / max(GROUPS - 1, 1))[:, None, None]
    return jnp.clip(0.15 * signal * both_gains * rough * ranged * level, -150.0, 150.0).astype(jnp.bfloat16)


def plant(array, key, low, top_value):
    longest = array.shape.index(max(array.shape))
    spots = []
    for shift in (0, 1):
        where = [jax.random.randint(jax.random.fold_in(key, axis), (), 0, length) for axis, length in enumerate(array.shape)]
        where[longest] = (where[longest] + shift) % array.shape[longest]
        spots.append(tuple(where))
    return array.at[spots[0]].set(low).at[spots[1]].set(top_value)


def setup_inputs(seed: int = 0) -> dict:
    seeds = jax.random.split(jax.random.key(seed), 4)
    snapshots = draw_snapshots(jax.random.fold_in(seeds[3], 71), 0)
    training = plant((jax.random.randint(seeds[1], (CELLS,), 0, 4) < 3).astype(jnp.int32), jax.random.fold_in(seeds[1], 1), 0, 1)
    doppler = plant(jax.random.randint(seeds[2], (GROUPS, BINS_G), 0, NDOPP), jax.random.fold_in(seeds[2], 1), 0, NDOPP - 1).astype(jnp.int32)
    return {"snapshots": snapshots, "training": training, "doppler": doppler}


load_ratio = 0.5
look_freq = 0.125

def steering(doppler):
    index = jnp.arange(CHANNELS * PULSES)
    chan = (index // PULSES).astype(jnp.float32)
    pulse = (index % PULSES).astype(jnp.float32)
    freq = doppler.astype(jnp.float32) / NDOPP - 0.5
    phase = 2.0 * jnp.pi * (look_freq * chan[:, None] + pulse[:, None] * freq[None, :])
    return jnp.concatenate([jnp.cos(phase), jnp.sin(phase)], 0) / jnp.sqrt(jnp.float32(DIM))

def complex_parts(gram):
    half = gram.shape[0] // 2
    upper = gram[:half, :half]
    cross = gram[:half, half:]
    lower = gram[half:, half:]
    return (upper + lower, cross.T - cross)

def filter_group(real_part, imag_part, noise, doppler, snaps):
    half = real_part.shape[0]
    loaded = real_part + load_ratio * noise * jnp.eye(half, dtype=jnp.float32)
    embed = jnp.concatenate([jnp.concatenate([loaded, -imag_part], 1), jnp.concatenate([imag_part, loaded], 1)], 0)
    factor = jnp.linalg.cholesky(embed)
    steer = steering(doppler)
    weights = jax.scipy.linalg.cho_solve((factor, True), steer)
    gain = lax.optimization_barrier(jnp.sum(steer * weights, axis=0))
    w_real = weights[:half] / gain[None, :]
    w_imag = weights[half:] / gain[None, :]
    taps = jnp.concatenate([jnp.concatenate([w_real, w_imag], 0), jnp.concatenate([-w_imag, w_real], 0)], 1).astype(jnp.bfloat16)
    result = lax.dot_general(taps.astype(jnp.float32), snaps.astype(jnp.float32), (((0,), (1,)), ((), ())), preferred_element_type=jnp.float32)
    return result.astype(jnp.bfloat16)

def reference(snapshots, training, doppler):
    keep = training.astype(jnp.bfloat16)[:, None]
    parts = []
    power = jnp.float32(0.0)
    for group in range(GROUPS):
        snaps = snapshots[group]
        gram = lax.dot_general((snaps * keep).astype(jnp.float32), snaps.astype(jnp.float32), (((0,), (0,)), ((), ())), preferred_element_type=jnp.float32)
        real_part, imag_part = complex_parts(gram)
        parts.append((real_part, imag_part))
        power = power + jnp.trace(real_part)
    noise = power / (GROUPS * DIM)
    outputs = []
    for group in range(GROUPS):
        outputs.append(filter_group(parts[group][0], parts[group][1], noise, doppler[group], snapshots[group]))
    return jnp.stack(outputs)
```

```python
import functools

import jax
import jax.numpy as jnp
from jax import lax
from jax.experimental import pallas as pl
from jax.experimental.pallas import tpu as pltpu
from jax.sharding import PartitionSpec as P

CHANNELS = 16
PULSES = 16
NDOPP = 1024


load_ratio = 0.5
look_freq = 0.125

EXTRA = 8
DONE = 0.99
REFINE = 2
HIGH = lax.Precision.HIGH
HIGHEST = lax.Precision.HIGHEST
MESH = pl.DeviceIdType.MESH


def steering(doppler, chans, pulses):
    index = jnp.arange(chans * pulses)
    chan = (index // pulses).astype(jnp.float32)
    pulse = (index % pulses).astype(jnp.float32)
    freq = doppler.astype(jnp.float32) / NDOPP - 0.5
    phase = 2.0 * jnp.pi * (look_freq * chan[:, None] + pulse[:, None] * freq[None, :])
    return jnp.concatenate([jnp.cos(phase), jnp.sin(phase)], 0) / jnp.sqrt(
        jnp.float32(chans * pulses)
    )


def gram_kernel(half, x_ref, keep_ref, out_ref, real_sum, cross_sum):
    step = pl.program_id(0)

    @pl.when(step == 0)
    def _():
        real_sum[...] = jnp.zeros_like(real_sum)
        cross_sum[...] = jnp.zeros_like(cross_sum)

    x = x_ref[...]
    keep = keep_ref[...].astype(jnp.bfloat16)
    masked = x.T * keep
    mr, mi = masked[:half], masked[half:]
    r, i = x[:, :half], x[:, half:]
    real_sum[...] += jnp.dot(
        jnp.concatenate([mr, mi], 1),
        jnp.concatenate([r, i], 0),
        preferred_element_type=jnp.float32,
    )
    cross_sum[...] += jnp.dot(mr, i, preferred_element_type=jnp.float32)

    @pl.when(step == pl.num_programs(0) - 1)
    def _():
        real = real_sum[...]
        cross = cross_sum[...]
        rows = lax.broadcasted_iota(jnp.int32, (half, half), 0)
        cols = lax.broadcasted_iota(jnp.int32, (half, half), 1)
        out_ref[...] = jnp.where(rows <= cols, real, cross.T - cross)


def gram(snaps, keep, block):
    cells, width = snaps.shape
    half = width // 2
    return pl.pallas_call(
        functools.partial(gram_kernel, half),
        grid=(cells // block,),
        in_specs=[
            pl.BlockSpec((block, width), lambda i: (i, 0)),
            pl.BlockSpec((1, block), lambda i: (0, i)),
        ],
        out_specs=pl.BlockSpec((half, half), lambda i: (0, 0)),
        out_shape=jax.ShapeDtypeStruct((half, half), jnp.float32),
        scratch_shapes=[
            pltpu.VMEM((half, half), jnp.float32),
            pltpu.VMEM((half, half), jnp.float32),
        ],
        name="gram",
    )(snaps, keep)


def sum_kernel(n, m, x_ref, out_ref, rs_buf, tr_src, tr_buf, mine, sems):
    me = lax.axis_index("cells")
    g = lax.axis_index("bins")
    half = x_ref.shape[0]
    rows = half // n
    rs_send, rs_recv, tr_send, tr_recv, ag_send, ag_recv = sems

    barrier = pltpu.get_barrier_semaphore()
    for k in range(1, n):
        pl.semaphore_signal(
            barrier, inc=1, device_id=(lax.rem(me + k, n), g), device_id_type=MESH
        )
    for k in range(1, m):
        pl.semaphore_signal(
            barrier, inc=1, device_id=(me, lax.rem(g + k, m)), device_id_type=MESH
        )
    pl.semaphore_wait(barrier, n + m - 2)

    copies = []
    for k in range(1, n):
        peer = lax.rem(me + k, n)
        copy = pltpu.make_async_remote_copy(
            src_ref=x_ref.at[pl.ds(pl.multiple_of(peer * rows, rows), rows)],
            dst_ref=rs_buf.at[k - 1],
            send_sem=rs_send.at[k - 1],
            recv_sem=rs_recv.at[k - 1],
            device_id=(peer, g),
            device_id_type=MESH,
        )
        copy.start()
        copies.append(copy)
    r = lax.broadcasted_iota(jnp.int32, (half, half), 0)
    c = lax.broadcasted_iota(jnp.int32, (half, half), 1)
    trace = jnp.sum(jnp.where(r == c, x_ref[...], 0.0), axis=0, keepdims=True)
    tr_src[...] = jnp.broadcast_to(trace, tr_src.shape)
    for k in range(1, m):
        copy = pltpu.make_async_remote_copy(
            src_ref=tr_src,
            dst_ref=tr_buf.at[k - 1],
            send_sem=tr_send.at[k - 1],
            recv_sem=tr_recv.at[k - 1],
            device_id=(me, lax.rem(g + k, m)),
            device_id_type=MESH,
        )
        copy.start()
        copies.append(copy)
    for copy in copies:
        copy.wait()
    total = x_ref[pl.ds(pl.multiple_of(me * rows, rows), rows), :]
    for k in range(n - 1):
        total = total + rs_buf[k]
    power = tr_src[...]
    for k in range(m - 1):
        power = power + tr_buf[k]
    mine[pl.ds(0, rows), :] = total
    mine[pl.ds(rows, EXTRA), :] = power
    out_ref[me] = jnp.concatenate([total, power], 0)

    copies = []
    for k in range(1, n):
        copy = pltpu.make_async_remote_copy(
            src_ref=mine,
            dst_ref=out_ref.at[me],
            send_sem=ag_send.at[k - 1],
            recv_sem=ag_recv.at[k - 1],
            device_id=(lax.rem(me + k, n), g),
            device_id_type=MESH,
        )
        copy.start()
        copies.append(copy)
    for k in range(1, n):
        copies[k - 1].wait_send()
        pltpu.make_async_remote_copy(
            src_ref=mine,
            dst_ref=out_ref.at[lax.rem(me + n - k, n)],
            send_sem=ag_send.at[k - 1],
            recv_sem=ag_recv.at[k - 1],
            device_id=(lax.rem(me + n - k, n), g),
            device_id_type=MESH,
        ).wait_recv()


def all_sum(packed):
    n, m = lax.axis_size("cells"), lax.axis_size("bins")
    half = packed.shape[0]
    rows = half // n
    dma = pltpu.SemaphoreType.DMA
    return pl.pallas_call(
        functools.partial(sum_kernel, n, m),
        out_shape=jax.ShapeDtypeStruct((n, rows + EXTRA, half), jnp.float32),
        in_specs=[pl.BlockSpec(memory_space=pltpu.VMEM)],
        out_specs=pl.BlockSpec(memory_space=pltpu.VMEM),
        scratch_shapes=[
            pltpu.VMEM((n - 1, rows, half), jnp.float32),
            pltpu.VMEM((EXTRA, half), jnp.float32),
            pltpu.VMEM((m - 1, EXTRA, half), jnp.float32),
            pltpu.VMEM((rows + EXTRA, half), jnp.float32),
            [dma((n - 1,)), dma((n - 1,)), dma((m - 1,)), dma((m - 1,)), dma((n - 1,)), dma((n - 1,))],
        ],
        compiler_params=pltpu.CompilerParams(collective_id=0, has_side_effects=True),
        name="all_sum",
    )(packed)


def newton_steps(ratio):
    d, steps = 1.0 / (ratio + 1.0), 0
    while d < DONE:
        d = (4.0 * d - 2.0 * d * d) / (1.0 + 2.0 * d - d * d)
        steps += 1
    return steps - 1


def solve_kernel(groups, parts_ref, steer_ref, taps_ref, mat, full, col):
    n = parts_ref.shape[0]
    rows = parts_ref.shape[1] - EXTRA
    half = parts_ref.shape[2]
    summed = jnp.concatenate([parts_ref[k, :rows, :] for k in range(n)], 0)
    power_row = parts_ref[0, rows:rows + 1, :]
    for k in range(1, n):
        power_row = power_row + parts_ref[k, rows:rows + 1, :]
    noise = jnp.sum(power_row, axis=1, keepdims=True) / (groups * half)
    low = load_ratio * noise
    r = lax.broadcasted_iota(jnp.int32, (half, half), 0)
    c = lax.broadcasted_iota(jnp.int32, (half, half), 1)
    flip = summed.T
    trace = jnp.sum(
        jnp.sum(jnp.where(r == c, summed, 0.0), axis=0, keepdims=True), axis=1, keepdims=True
    )
    eye = jnp.where(r == c, 1.0, 0.0)
    scale = 1.0 / (0.5 * trace + low)
    real = (jnp.where(r <= c, summed, flip) + low * eye) * scale
    imag = jnp.where(r > c, summed, jnp.where(r < c, -flip, 0.0)) * scale
    mat[:half, :half] = real
    mat[half:, half:] = real
    mat[:half, half:] = -imag
    mat[half:, :half] = imag

    def put(xr, xi):
        col[:half, :] = xr
        col[half:, :] = xi
        full[:half, :half] = xr
        full[half:, half:] = xr
        full[:half, half:] = -xi
        full[half:, :half] = xi

    d = low * scale
    bend = 2.0 / (1.0 + 2.0 * d - d * d)
    d = (4.0 * d - 2.0 * d * d) / (1.0 + 2.0 * d - d * d)
    put(bend * (2.0 * eye - real), -bend * imag)

    def newton(_, d):
        left = jnp.dot(mat[...], col[...], preferred_element_type=jnp.float32, precision=HIGH)
        bend = 2.0 / (1.0 + 2.0 * d - d * d)
        step = jnp.dot(
            full[...],
            jnp.concatenate([2.0 * eye - left[:half], -left[half:]], 0),
            preferred_element_type=jnp.float32,
            precision=HIGH,
        )
        put(bend * step[:half], bend * step[half:])
        return (4.0 * d - 2.0 * d * d) / (1.0 + 2.0 * d - d * d)

    lax.fori_loop(0, newton_steps(groups * half), newton, d)

    steer = steer_ref[...]
    w = jnp.dot(full[...], steer, preferred_element_type=jnp.float32, precision=HIGH)
    for _ in range(REFINE):
        gap = steer - jnp.dot(mat[...], w, preferred_element_type=jnp.float32, precision=HIGHEST)
        w = w + jnp.dot(full[...], gap, preferred_element_type=jnp.float32, precision=HIGH)
    w = w * scale
    gain = jnp.sum(steer * w, axis=0, keepdims=True)
    wr = (w[:half] / gain).T
    wi = (w[half:] / gain).T
    bins = wr.shape[0]
    taps_ref[:bins, :half] = wr.astype(jnp.bfloat16)
    taps_ref[:bins, half:] = wi.astype(jnp.bfloat16)
    taps_ref[bins:, :half] = (-wi).astype(jnp.bfloat16)
    taps_ref[bins:, half:] = wr.astype(jnp.bfloat16)


def solve(parts, steer, groups):
    half = parts.shape[2]
    bins = steer.shape[1]
    return pl.pallas_call(
        functools.partial(solve_kernel, groups),
        out_shape=jax.ShapeDtypeStruct((2 * bins, 2 * half), jnp.bfloat16),
        in_specs=[pl.BlockSpec(memory_space=pltpu.VMEM)] * 2,
        out_specs=pl.BlockSpec(memory_space=pltpu.VMEM),
        scratch_shapes=[
            pltpu.VMEM((2 * half, 2 * half), jnp.float32),
            pltpu.VMEM((2 * half, 2 * half), jnp.float32),
            pltpu.VMEM((2 * half, half), jnp.float32),
        ],
        name="solve",
    )(parts, steer)


def filter_kernel(taps_ref, x_ref, out_ref):
    out_ref[...] = lax.dot_general(
        taps_ref[...], x_ref[...], (((1,), (1,)), ((), ())), preferred_element_type=jnp.float32
    ).astype(out_ref.dtype)


def apply_taps(taps, snaps, block):
    cells, width = snaps.shape
    rows = taps.shape[0]
    return pl.pallas_call(
        filter_kernel,
        grid=(cells // block,),
        in_specs=[
            pl.BlockSpec((rows, width), lambda i: (0, 0)),
            pl.BlockSpec((block, width), lambda i: (i, 0)),
        ],
        out_specs=pl.BlockSpec((rows, block), lambda i: (0, i)),
        out_shape=jax.ShapeDtypeStruct((rows, cells), jnp.bfloat16),
        name="filter",
    )(taps, snaps)


def per_device(snapshots, training, doppler):
    snaps = snapshots[0]
    block = min(1024, snaps.shape[0])
    packed = gram(snaps, training[None, :], block)
    parts = all_sum(packed)
    steer = steering(doppler[0], CHANNELS, PULSES)
    taps = solve(parts, steer, lax.axis_size("bins"))
    return apply_taps(taps, snaps, block)[None]


def solution(mesh):
    in_specs = (P("bins", "cells", None), P("cells"), P("bins", None))
    out_specs = P("bins", None, "cells")
    return jax.shard_map(
        per_device, mesh=mesh, in_specs=in_specs, out_specs=out_specs, check_vma=False
    )
```

```python
import functools

import jax
import jax.numpy as jnp
from jax import lax
from jax.experimental import pallas as pl
from jax.experimental.pallas import tpu as pltpu
from jax.sharding import PartitionSpec as P

CHANNELS = 16
PULSES = 16
NDOPP = 1024


load_ratio = 0.5
look_freq = 0.125

EXTRA = 8
DONE = 0.99
REFINE = 2
HIGH = lax.Precision.HIGH
HIGHEST = lax.Precision.HIGHEST
MESH = pl.DeviceIdType.MESH


def steering(doppler, chans, pulses):
    index = jnp.arange(chans * pulses)
    chan = (index // pulses).astype(jnp.float32)
    pulse = (index % pulses).astype(jnp.float32)
    freq = doppler.astype(jnp.float32) / NDOPP - 0.5
    phase = 2.0 * jnp.pi * (look_freq * chan[:, None] + pulse[:, None] * freq[None, :])
    return jnp.concatenate([jnp.cos(phase), jnp.sin(phase)], 0) / jnp.sqrt(
        jnp.float32(chans * pulses)
    )


def gram_kernel(half, x_ref, keep_ref, out_ref, real_sum, cross_sum):
    step = pl.program_id(0)

    @pl.when(step == 0)
    def _():
        real_sum[...] = jnp.zeros_like(real_sum)
        cross_sum[...] = jnp.zeros_like(cross_sum)

    x = x_ref[...]
    keep = keep_ref[...].astype(jnp.bfloat16)
    masked = x.T * keep
    mr, mi = masked[:half], masked[half:]
    r, i = x[:, :half], x[:, half:]
    real_sum[...] += jnp.dot(
        jnp.concatenate([mr, mi], 1),
        jnp.concatenate([r, i], 0),
        preferred_element_type=jnp.float32,
    )
    cross_sum[...] += jnp.dot(mr, i, preferred_element_type=jnp.float32)

    @pl.when(step == pl.num_programs(0) - 1)
    def _():
        real = real_sum[...]
        cross = cross_sum[...]
        rows = lax.broadcasted_iota(jnp.int32, (half, half), 0)
        cols = lax.broadcasted_iota(jnp.int32, (half, half), 1)
        out_ref[...] = jnp.where(rows <= cols, real, cross.T - cross)


def gram(snaps, keep, block):
    cells, width = snaps.shape
    half = width // 2
    return pl.pallas_call(
        functools.partial(gram_kernel, half),
        grid=(cells // block,),
        in_specs=[
            pl.BlockSpec((block, width), lambda i: (i, 0)),
            pl.BlockSpec((1, block), lambda i: (0, i)),
        ],
        out_specs=pl.BlockSpec((half, half), lambda i: (0, 0)),
        out_shape=jax.ShapeDtypeStruct((half, half), jnp.float32),
        scratch_shapes=[
            pltpu.VMEM((half, half), jnp.float32),
            pltpu.VMEM((half, half), jnp.float32),
        ],
        name="gram",
    )(snaps, keep)


def sum_kernel(n, m, x_ref, out_ref, rs_buf, tr_src, tr_buf, mine, sems):
    me = lax.axis_index("cells")
    g = lax.axis_index("bins")
    half = x_ref.shape[0]
    rows = half // n
    rs_send, rs_recv, tr_send, tr_recv, ag_send, ag_recv = sems

    barrier = pltpu.get_barrier_semaphore()
    for k in range(1, n):
        pl.semaphore_signal(
            barrier, inc=1, device_id=(lax.rem(me + k, n), g), device_id_type=MESH
        )
    for k in range(1, m):
        pl.semaphore_signal(
            barrier, inc=1, device_id=(me, lax.rem(g + k, m)), device_id_type=MESH
        )
    pl.semaphore_wait(barrier, n + m - 2)

    copies = []
    for k in range(1, n):
        peer = lax.rem(me + k, n)
        copy = pltpu.make_async_remote_copy(
            src_ref=x_ref.at[pl.ds(pl.multiple_of(peer * rows, rows), rows)],
            dst_ref=rs_buf.at[k - 1],
            send_sem=rs_send.at[k - 1],
            recv_sem=rs_recv.at[k - 1],
            device_id=(peer, g),
            device_id_type=MESH,
        )
        copy.start()
        copies.append(copy)
    r = lax.broadcasted_iota(jnp.int32, (half, half), 0)
    c = lax.broadcasted_iota(jnp.int32, (half, half), 1)
    trace = jnp.sum(jnp.where(r == c, x_ref[...], 0.0), axis=0, keepdims=True)
    tr_src[...] = jnp.broadcast_to(trace, tr_src.shape)
    for k in range(1, m):
        copy = pltpu.make_async_remote_copy(
            src_ref=tr_src,
            dst_ref=tr_buf.at[k - 1],
            send_sem=tr_send.at[k - 1],
            recv_sem=tr_recv.at[k - 1],
            device_id=(me, lax.rem(g + k, m)),
            device_id_type=MESH,
        )
        copy.start()
        copies.append(copy)
    for copy in copies:
        copy.wait()
    total = x_ref[pl.ds(pl.multiple_of(me * rows, rows), rows), :]
    for k in range(n - 1):
        total = total + rs_buf[k]
    power = tr_src[...]
    for k in range(m - 1):
        power = power + tr_buf[k]
    mine[pl.ds(0, rows), :] = total
    mine[pl.ds(rows, EXTRA), :] = power
    out_ref[me] = jnp.concatenate([total, power], 0)

    copies = []
    for k in range(1, n):
        copy = pltpu.make_async_remote_copy(
            src_ref=mine,
            dst_ref=out_ref.at[me],
            send_sem=ag_send.at[k - 1],
            recv_sem=ag_recv.at[k - 1],
            device_id=(lax.rem(me + k, n), g),
            device_id_type=MESH,
        )
        copy.start()
        copies.append(copy)
    for k in range(1, n):
        copies[k - 1].wait_send()
        pltpu.make_async_remote_copy(
            src_ref=mine,
            dst_ref=out_ref.at[lax.rem(me + n - k, n)],
            send_sem=ag_send.at[k - 1],
            recv_sem=ag_recv.at[k - 1],
            device_id=(lax.rem(me + n - k, n), g),
            device_id_type=MESH,
        ).wait_recv()


def all_sum(packed):
    n, m = lax.axis_size("cells"), lax.axis_size("bins")
    half = packed.shape[0]
    rows = half // n
    dma = pltpu.SemaphoreType.DMA
    return pl.pallas_call(
        functools.partial(sum_kernel, n, m),
        out_shape=jax.ShapeDtypeStruct((n, rows + EXTRA, half), jnp.float32),
        in_specs=[pl.BlockSpec(memory_space=pltpu.VMEM)],
        out_specs=pl.BlockSpec(memory_space=pltpu.VMEM),
        scratch_shapes=[
            pltpu.VMEM((n - 1, rows, half), jnp.float32),
            pltpu.VMEM((EXTRA, half), jnp.float32),
            pltpu.VMEM((m - 1, EXTRA, half), jnp.float32),
            pltpu.VMEM((rows + EXTRA, half), jnp.float32),
            [dma((n - 1,)), dma((n - 1,)), dma((m - 1,)), dma((m - 1,)), dma((n - 1,)), dma((n - 1,))],
        ],
        compiler_params=pltpu.CompilerParams(collective_id=0, has_side_effects=True),
        name="all_sum",
    )(packed)


def newton_steps(ratio):
    d, steps = 1.0 / (ratio + 1.0), 0
    while d < DONE:
        d = (4.0 * d - 2.0 * d * d) / (1.0 + 2.0 * d - d * d)
        steps += 1
    return steps - 1


def solve_kernel(groups, parts_ref, steer_ref, taps_ref, mat, full, col):
    n = parts_ref.shape[0]
    rows = parts_ref.shape[1] - EXTRA
    half = parts_ref.shape[2]
    summed = jnp.concatenate([parts_ref[k, :rows, :] for k in range(n)], 0)
    power_row = parts_ref[0, rows:rows + 1, :]
    for k in range(1, n):
        power_row = power_row + parts_ref[k, rows:rows + 1, :]
    noise = jnp.sum(power_row, axis=1, keepdims=True) / (groups * half)
    low = load_ratio * noise
    r = lax.broadcasted_iota(jnp.int32, (half, half), 0)
    c = lax.broadcasted_iota(jnp.int32, (half, half), 1)
    flip = summed.T
    trace = jnp.sum(
        jnp.sum(jnp.where(r == c, summed, 0.0), axis=0, keepdims=True), axis=1, keepdims=True
    )
    eye = jnp.where(r == c, 1.0, 0.0)
    scale = 1.0 / (0.5 * trace + low)
    real = (jnp.where(r <= c, summed, flip) + low * eye) * scale
    imag = jnp.where(r > c, summed, jnp.where(r < c, -flip, 0.0)) * scale
    mat[:half, :half] = real
    mat[half:, half:] = real
    mat[:half, half:] = -imag
    mat[half:, :half] = imag

    def put(xr, xi):
        col[:half, :] = xr
        col[half:, :] = xi
        full[:half, :half] = xr
        full[half:, half:] = xr
        full[:half, half:] = -xi
        full[half:, :half] = xi

    d = low * scale
    bend = 2.0 / (1.0 + 2.0 * d - d * d)
    d = (4.0 * d - 2.0 * d * d) / (1.0 + 2.0 * d - d * d)
    put(bend * (2.0 * eye - real), -bend * imag)

    def newton(_, d):
        left = jnp.dot(mat[...], col[...], preferred_element_type=jnp.float32, precision=HIGH)
        bend = 2.0 / (1.0 + 2.0 * d - d * d)
        step = jnp.dot(
            full[...],
            jnp.concatenate([2.0 * eye - left[:half], -left[half:]], 0),
            preferred_element_type=jnp.float32,
            precision=HIGH,
        )
        put(bend * step[:half], bend * step[half:])
        return (4.0 * d - 2.0 * d * d) / (1.0 + 2.0 * d - d * d)

    lax.fori_loop(0, newton_steps(groups * half), newton, d)

    steer = steer_ref[...]
    w = jnp.dot(full[...], steer, preferred_element_type=jnp.float32, precision=HIGH)
    for _ in range(REFINE):
        gap = steer - jnp.dot(mat[...], w, preferred_element_type=jnp.float32, precision=HIGHEST)
        w = w + jnp.dot(full[...], gap, preferred_element_type=jnp.float32, precision=HIGH)
    w = w * scale
    gain = jnp.sum(steer * w, axis=0, keepdims=True)
    wr = (w[:half] / gain).T
    wi = (w[half:] / gain).T
    bins = wr.shape[0]
    taps_ref[:bins, :half] = wr.astype(jnp.bfloat16)
    taps_ref[:bins, half:] = wi.astype(jnp.bfloat16)
    taps_ref[bins:, :half] = (-wi).astype(jnp.bfloat16)
    taps_ref[bins:, half:] = wr.astype(jnp.bfloat16)


def solve(parts, steer, groups):
    half = parts.shape[2]
    bins = steer.shape[1]
    return pl.pallas_call(
        functools.partial(solve_kernel, groups),
        out_shape=jax.ShapeDtypeStruct((2 * bins, 2 * half), jnp.bfloat16),
        in_specs=[pl.BlockSpec(memory_space=pltpu.VMEM)] * 2,
        out_specs=pl.BlockSpec(memory_space=pltpu.VMEM),
        scratch_shapes=[
            pltpu.VMEM((2 * half, 2 * half), jnp.float32),
            pltpu.VMEM((2 * half, 2 * half), jnp.float32),
            pltpu.VMEM((2 * half, half), jnp.float32),
        ],
        name="solve",
    )(parts, steer)


def filter_kernel(taps_ref, x_ref, out_ref):
    out_ref[...] = lax.dot_general(
        taps_ref[...], x_ref[...], (((1,), (1,)), ((), ())), preferred_element_type=jnp.float32
    ).astype(out_ref.dtype)


def apply_taps(taps, snaps, block):
    cells, width = snaps.shape
    rows = taps.shape[0]
    return pl.pallas_call(
        filter_kernel,
        grid=(cells // block,),
        in_specs=[
            pl.BlockSpec((rows, width), lambda i: (0, 0)),
            pl.BlockSpec((block, width), lambda i: (i, 0)),
        ],
        out_specs=pl.BlockSpec((rows, block), lambda i: (0, i)),
        out_shape=jax.ShapeDtypeStruct((rows, cells), jnp.bfloat16),
        name="filter",
    )(taps, snaps)


def per_device(snapshots, training, doppler):
    snaps = snapshots[0]
    block = min(4096, snaps.shape[0])
    packed = gram(snaps, training[None, :], block)
    parts = all_sum(packed)
    steer = steering(doppler[0], CHANNELS, PULSES)
    taps = solve(parts, steer, lax.axis_size("bins"))
    return apply_taps(taps, snaps, block)[None]


def solution(mesh):
    in_specs = (P("bins", "cells", None), P("cells"), P("bins", None))
    out_specs = P("bins", None, "cells")
    return jax.shard_map(
        per_device, mesh=mesh, in_specs=in_specs, out_specs=out_specs, check_vma=False
    )
```
